32 devices in a mesh: expert: 32 (over z, y, x, core).
Axes of the slice: x: 2, y: 2, z: 4, core: 2. Of those that a mesh axis runs over, the one named last changes fastest.
Arguments:
- routed_rows: bfloat16 [6144, 2048], P('expert'), may hold values from -6 to 6
- expert_index: int32 [6144, 1], P('expert'), may hold values from 0 to 31; in each aligned block of 192 rows (0 to 191, 192 to 383, ...) at most 12 rows name the same one
- route_weight: float32 [6144], P('expert'), may hold values from 0.1 to 1
- cotangent: bfloat16 [6144, 2048], P('expert'), may hold values from -6 to 6
- gate_weight: bfloat16 [32, 2048, 768], P('expert'), may hold values from -0.125 to 0.125
- up_weight: bfloat16 [32, 2048, 768], P('expert'), may hold values from -0.125 to 0.125
- down_weight: bfloat16 [32, 768, 2048], P('expert'), may hold values from -0.21875 to 0.21875
Outputs:
- layer_out: bfloat16 [6144, 2048], P('expert')
- row_grad: bfloat16 [6144, 2048], P('expert')
- weight_grad: float32 [6144], P('expert')
- gate_grad: bfloat16 [32, 2048, 768], P('expert')
- up_grad: bfloat16 [32, 2048, 768], P('expert')
- down_grad: bfloat16 [32, 768, 2048], P('expert')
The draws below stay inside these ranges and needn't reach their ends.
Inputs may be any that keep to these rules, and one draw needn't show every extreme that they name: `expert_index`: among the 192 rows of one device no expert is named more than 12 times, a bound that some block reaches.
All inputs are finite; a program needn't handle non-finite values.
Results may differ from the reference program's by a relative error of at most 0.0058.
Values may be sent and summed in bfloat16 or wider, within the bound.
A program may use at most 128 MiB of HBM per device.

```python
import math
import jax
import jax.numpy as jnp
import numpy as np
from jax import lax

D = 2048
FF = 768
ROW_DEV = 192
EXPERTS = 32
ROWS = 6144
CAP = 12
N_EXPERT = 32


def steps_of(rng, extent, pieces, low, largest):
    def one(dim, parts):
        draws = jax.random.uniform(jax.random.fold_in(jax.random.fold_in(rng, 6), dim), (parts,), jnp.float32, low / len(pieces), largest / len(pieces))
        return jnp.repeat(jnp.exp(draws), extent[dim] // parts).reshape((-1,) + (1,) * (len(extent) - dim - 1))

    gain = one(*pieces[0])
    for cut in pieces[1:]:
        gain = gain * one(*cut)
    return gain


def shared_out(own_key, own, number, rows, number_of, top, limit, skew):
    sequence = jax.random.permutation(own_key, number_of)
    heavy_load, ordinary = shares(number_of, rows * top, limit, skew, True), shares(number_of, rows * top, limit, skew, False)
    places = jnp.arange(number_of)

    def named(lengths, turn):
        used = int((lengths > 0).sum())
        fixed = max(1, used // 4)
        moved = fixed + (places - fixed + turn * (used - fixed)) % max(1, number_of - fixed)
        return jnp.zeros((number_of,), jnp.int32).at[sequence[jnp.where(places < fixed, places, moved)]].set(jnp.asarray(lengths, jnp.int32))

    lengths = jnp.where(number % 4 == 0, named(heavy_load, number // 4), named(ordinary, number - number // 4 - 1))
    mixed = jax.random.permutation(jax.random.fold_in(own, 3), number_of)
    donor, receiver = mixed[0:number_of // 2 * 2:2], mixed[1:number_of // 2 * 2:2]
    margin = jnp.minimum(lengths[donor] - 1, limit - lengths[receiver]) // 2
    margin = jnp.where((donor == sequence[0]) | (receiver == sequence[0]) | (lengths[receiver] == 0), 0, jnp.maximum(margin, 0))
    moved = jax.random.randint(jax.random.fold_in(own, 4), (number_of // 2,), 0, 1 << 20) % (margin + 1)
    lengths = lengths.at[donor].add(-moved).at[receiver].add(moved)
    labels = jnp.searchsorted(jnp.cumsum(lengths), jnp.arange(rows * top), side="right").astype(jnp.int32)
    grid = labels.reshape(top, rows).T
    grid = grid[jax.random.permutation(jax.random.fold_in(own, 1), rows)]
    turn = jax.random.randint(jax.random.fold_in(own, 2), (rows, 1), 0, top)
    return jnp.take_along_axis(grid, (jnp.arange(top)[None, :] + turn) % top, axis=1)


def shares(amount, total, limit, slope, full):
    weights = [(1 << 20) // math.isqrt(rank ** slope) + 1 for rank in range(1, amount + 1)]
    largest = limit if full else min(limit, max(-(-total // amount), total * weights[0] // sum(weights)))
    least = 1 if total - largest >= amount - 1 else 0
    given, rest = [largest] + [least] * (amount - 1), total - largest - least * (amount - 1)
    while rest > 0:
        free = [i for i in range(1, amount) if given[i] < largest] or [i for i in range(1, amount) if given[i] < limit]
        pool, budget = sum([weights[i] for i in free]), rest
        for i in free:
            more = min(limit - given[i], max(1, budget * weights[i] // pool), rest)
            given[i] = given[i] + more
            rest = rest - more
    return np.array(given)


def scatter_about(own_key, extent, width, most, shards=(), held_as=jnp.bfloat16):
    values = jax.random.normal(own_key, extent, jnp.float32) * width
    if len(shards) > 0:
        values = steps_of(own_key, extent, shards, -0.22, 0.18) * values
    return jnp.clip(values, min=-most, max=most).astype(held_as)


def setup_inputs(seed: int = 0) -> dict:
    arg_keys = jax.random.split(jax.random.key(seed), 8)
    routed_rows = scatter_about(arg_keys[0], (ROWS, D), 1.0, 6.0, ((0, 32),))
    expert_index_keys = jax.random.split(jax.random.fold_in(arg_keys[1], 1), ROWS // ROW_DEV)
    expert_index_turns = jax.random.permutation(jax.random.fold_in(arg_keys[1], 3), ROWS // ROW_DEV)
    expert_index = jax.vmap(lambda own, number: shared_out(jax.random.fold_in(arg_keys[1], 2), own, number, ROW_DEV, EXPERTS, 1, CAP, 2))(expert_index_keys, expert_index_turns).reshape((ROWS, 1))
    route_weight = jnp.clip(jnp.exp(math.log(1.0) - 2.3025851 * jax.random.uniform(arg_keys[2], (ROWS,), jnp.float32) ** steps_of(arg_keys[2], (ROWS,), ((0, 32),), -0.2, 0.2)), 0.1, 1.0)
    cotangent = scatter_about(arg_keys[3], (ROWS, D), 1.0, 6.0, ((0, 32),))
    gate_weight = scatter_about(arg_keys[4], (EXPERTS, D, FF), D ** -0.5, 0.125, ((0, 32),))
    up_weight = scatter_about(arg_keys[5], (EXPERTS, D, FF), D ** -0.5, 0.125, ((0, 32),))
    down_weight = scatter_about(arg_keys[6], (EXPERTS, FF, D), FF ** -0.5, 0.21875, ((0, 32),))
    return dict(routed_rows=routed_rows, expert_index=expert_index, route_weight=route_weight, cotangent=cotangent, gate_weight=gate_weight, up_weight=up_weight, down_weight=down_weight)


def expert_pass(inputs):
    rows_in, out_grad, w_gate, w_up, w_down = inputs
    gate_act = jnp.dot(rows_in, w_gate, preferred_element_type=jnp.float32)
    up_act = jnp.dot(rows_in, w_up, preferred_element_type=jnp.float32)
    sigma = jax.nn.sigmoid(gate_act)
    silu_gate = gate_act * sigma
    hidden = (silu_gate * up_act).astype(jnp.bfloat16)
    expert_out = jnp.dot(hidden, w_down, preferred_element_type=jnp.float32).astype(jnp.bfloat16)
    hidden_grad = jnp.dot(out_grad, w_down.T, preferred_element_type=jnp.float32)
    gate_pre = (hidden_grad * up_act * sigma * (1.0 + gate_act * (1.0 - sigma))).astype(jnp.bfloat16)
    up_pre = (hidden_grad * silu_gate).astype(jnp.bfloat16)
    input_grad = (jnp.dot(gate_pre, w_gate.T, preferred_element_type=jnp.float32)
                  + jnp.dot(up_pre, w_up.T, preferred_element_type=jnp.float32)).astype(jnp.bfloat16)
    gate_grad = jnp.dot(rows_in.T, gate_pre, preferred_element_type=jnp.float32).astype(jnp.bfloat16)
    up_grad = jnp.dot(rows_in.T, up_pre, preferred_element_type=jnp.float32).astype(jnp.bfloat16)
    down_grad = jnp.dot(hidden.T, out_grad, preferred_element_type=jnp.float32).astype(jnp.bfloat16)
    return expert_out, input_grad, gate_grad, up_grad, down_grad


def reference(routed_rows, expert_index, route_weight, cotangent, gate_weight, up_weight, down_weight):
    choice_ids = expert_index[:, 0]
    devices = N_EXPERT
    per_expert = devices * CAP
    onehot = (choice_ids[:, None] == jnp.arange(EXPERTS, dtype=jnp.int32)[None, :]).astype(jnp.int32)
    stacked = onehot.reshape(devices, ROW_DEV, EXPERTS)
    earlier = jnp.cumsum(stacked, axis=1) - stacked
    rank_within = jnp.sum(earlier * stacked, axis=2).reshape(-1).astype(jnp.int32)
    source = (jnp.arange(ROWS, dtype=jnp.int32) // ROW_DEV).astype(jnp.int32)
    slot_index = (choice_ids * per_expert + source * CAP + rank_within).astype(jnp.int32)
    out_grad = (route_weight[:, None] * cotangent.astype(jnp.float32)).astype(jnp.bfloat16)
    buffer_in = jnp.zeros((EXPERTS * per_expert, D), jnp.bfloat16).at[slot_index].set(routed_rows)
    buffer_grad = jnp.zeros((EXPERTS * per_expert, D), jnp.bfloat16).at[slot_index].set(out_grad)
    results = lax.map(expert_pass, (buffer_in.reshape(EXPERTS, per_expert, D),
                                    buffer_grad.reshape(EXPERTS, per_expert, D),
                                    gate_weight, up_weight, down_weight))
    expert_out, input_grad, gate_grad, up_grad, down_grad = results
    out_rows = expert_out.reshape(-1, D)[slot_index]
    row_grad = input_grad.reshape(-1, D)[slot_index]
    layer_out = (route_weight[:, None] * out_rows.astype(jnp.float32)).astype(jnp.bfloat16)
    weight_grad = jnp.sum(cotangent.astype(jnp.float32) * out_rows.astype(jnp.float32), axis=1)
    return layer_out, row_grad, weight_grad, gate_grad, up_grad, down_grad
```

```python
import functools
import math

import jax
import jax.numpy as jnp
from jax import lax
from jax.experimental import pallas as pl
from jax.experimental.pallas import tpu as pltpu
from jax.sharding import PartitionSpec as P

F32 = jnp.float32
BF16 = jnp.bfloat16
SUB = 16
NT = (((1,), (1,)), ((), ()))
TN = (((0,), (0,)), ((), ()))


def dot(a, b):
    return jnp.dot(a, b, preferred_element_type=F32)


def kernel(
    n, cap, part, tile,
    idx_row, idx_col, weight_col, rows, cot, wg_any, wu_any, wd_any,
    layer, row_grad, weight_grad, rin_any, og_any, hid_any, gp_any, up_any,
    wg, wu, wd, send, recv, rin, og, ga, ua, hid, gp, up, eo,
    load_sem, store_sem, send_sem, recv_sem, own_sem,
):
    me = lax.axis_index("expert")
    groups = SUB // part
    blocks = cap // part
    row_count, width = rows.shape
    chunk = width // groups
    some = math.gcd(n, 32)
    wide = some * SUB
    narrow = some * part
    hidden_units = wg.shape[1]

    loads = [
        pltpu.make_async_copy(src, dst, load_sem.at[i])
        for i, (src, dst) in enumerate(((wg_any, wg), (wu_any, wu), (wd_any, wd)))
    ]
    for load in loads:
        load.start()

    barrier = pltpu.get_barrier_semaphore()

    @pl.loop(1, n)
    def _(s):
        pl.semaphore_signal(
            barrier, inc=1, device_id=(lax.rem(me + s, n),), device_id_type=pl.DeviceIdType.MESH
        )

    choice_row = idx_row[...]
    hot_row = (lax.broadcasted_iota(jnp.int32, (n, row_count), 0) == choice_row).astype(F32)
    before = (
        lax.broadcasted_iota(jnp.int32, (row_count, row_count), 0)
        < lax.broadcasted_iota(jnp.int32, (row_count, row_count), 1)
    ).astype(F32)
    rank_row = jnp.sum(dot(hot_row, before) * hot_row, axis=0, keepdims=True).astype(jnp.int32)
    choice_col = idx_col[...]
    hot_col = (lax.broadcasted_iota(jnp.int32, (row_count, n), 1) == choice_col).astype(F32)
    after = (
        lax.broadcasted_iota(jnp.int32, (row_count, row_count), 0)
        > lax.broadcasted_iota(jnp.int32, (row_count, row_count), 1)
    ).astype(F32)
    rank_col = jnp.sum(dot(after, hot_col) * hot_col, axis=1, keepdims=True).astype(jnp.int32)

    def place(choice, rank, q):
        off = rank - q * part
        return jnp.where((off >= 0) & (off < part), choice * SUB + off, -SUB * n)

    def columns(c):
        return slice(c * chunk, (c + 1) * chunk)

    def dispatch(p, source):
        @pl.loop(0, n // some)
        def _(b):
            at = pl.ds(pl.multiple_of(b * wide, wide), wide)
            for q in range(blocks):
                base = place(choice_row, rank_row, q) - b * wide
                total = None
                for c in range(groups):
                    table = (
                        lax.broadcasted_iota(jnp.int32, (wide, row_count), 0) == base + c * part
                    ).astype(F32).astype(BF16)
                    term = dot(table, source(c))
                    total = term if total is None else total + term
                send[p, at, columns(q)] = total.astype(BF16)

    def slab(d):
        return pl.ds(pl.multiple_of(d * SUB, SUB), SUB)

    def ship(p):
        own = pltpu.make_async_copy(
            send.at[p, slab(me)], recv.at[p, slab(me)], own_sem.at[p]
        )

        @pl.loop(0, n)
        def _(s):
            to = lax.rem(me + n // 2 + s, n)

            @pl.when(to != me)
            def _():
                pltpu.make_async_remote_copy(
                    src_ref=send.at[p, slab(to)],
                    dst_ref=recv.at[p, slab(me)],
                    send_sem=send_sem.at[p],
                    recv_sem=recv_sem.at[p],
                    device_id=(to,),
                    device_id_type=pl.DeviceIdType.MESH,
                ).start()

        own.start()
        return own

    def arrived(p, own):
        own.wait()
        most = recv.at[p, pl.ds(0, (n - 1) * SUB)]
        pltpu.make_async_copy(most, most, recv_sem.at[p]).wait()

    def left(p):
        most = send.at[p, pl.ds(0, (n - 1) * SUB)]
        pltpu.make_async_copy(most, most, send_sem.at[p]).wait()

    def pick(c):
        row = lax.broadcasted_iota(jnp.int32, (narrow, wide), 0)
        col = lax.broadcasted_iota(jnp.int32, (narrow, wide), 1)
        low = row & (part - 1)
        return (col == (row - low) * groups + c * part + low).astype(F32).astype(BF16)

    def spread(c):
        row = lax.broadcasted_iota(jnp.int32, (wide, narrow), 0)
        col = lax.broadcasted_iota(jnp.int32, (wide, narrow), 1)
        low = col & (part - 1)
        return (row == (col - low) * groups + c * part + low).astype(F32).astype(BF16)

    def unpack(p, into):
        @pl.loop(0, n // some)
        def _(b):
            at = pl.ds(pl.multiple_of(b * wide, wide), wide)
            for c in range(groups):
                table = pick(c)
                for q in range(blocks):
                    to = pl.ds(pl.multiple_of(q * n * part + b * narrow, narrow), narrow)
                    into[to, columns(c)] = dot(table, recv[p, at, columns(q)]).astype(BF16)

    def pack(p):
        @pl.loop(0, n // some)
        def _(b):
            at = pl.ds(pl.multiple_of(b * wide, wide), wide)
            for q in range(blocks):
                to = pl.ds(pl.multiple_of(q * n * part + b * narrow, narrow), narrow)
                total = None
                for c in range(groups):
                    term = dot(spread(c), eo[to, columns(c)])
                    total = term if total is None else total + term
                send[p, at, columns(q)] = total.astype(BF16)

    def combine(p, c):
        total = None
        for b in range(n // some):
            for q in range(blocks):
                base = place(choice_col, rank_col, q) + c * part - b * wide
                table = (
                    lax.broadcasted_iota(jnp.int32, (row_count, wide), 1) == base
                ).astype(F32).astype(BF16)
                term = dot(table, recv[p, b * wide:(b + 1) * wide, columns(q)])
                total = term if total is None else total + term
        return total

    weight = weight_col[...]
    dispatch(0, lambda c: rows[:, columns(c)])
    pl.semaphore_wait(barrier, n - 1)
    own_a = ship(0)
    dispatch(1, lambda c: (weight * cot[:, columns(c)].astype(F32)).astype(BF16))
    own_b = ship(1)
    for load in loads:
        load.wait()

    arrived(0, own_a)
    unpack(0, rin)

    @pl.loop(0, hidden_units // tile)
    def _(t):
        at = pl.ds(pl.multiple_of(t * tile, tile), tile)
        gate = dot(rin[...], wg[:, at])
        upper = dot(rin[...], wu[:, at])
        ga[:, at] = gate
        ua[:, at] = upper
        hid[:, at] = (gate * jax.nn.sigmoid(gate) * upper).astype(BF16)

    @pl.loop(0, width // tile)
    def _(t):
        at = pl.ds(pl.multiple_of(t * tile, tile), tile)
        eo[:, at] = dot(hid[...], wd[:, at]).astype(BF16)

    pack(2)
    own_c = ship(2)

    arrived(1, own_b)
    unpack(1, og)

    @pl.loop(0, hidden_units // tile)
    def _(t):
        at = pl.ds(pl.multiple_of(t * tile, tile), tile)
        grad = lax.dot_general(og[...], wd[at, :], NT, preferred_element_type=F32)
        gate = ga[:, at]
        sigma = jax.nn.sigmoid(gate)
        gp[:, at] = (grad * ua[:, at] * sigma * (1.0 + gate * (1.0 - sigma))).astype(BF16)
        up[:, at] = (grad * (gate * sigma)).astype(BF16)

    @pl.loop(0, width // tile)
    def _(t):
        at = pl.ds(pl.multiple_of(t * tile, tile), tile)
        eo[:, at] = (
            lax.dot_general(gp[...], wg[at, :], NT, preferred_element_type=F32)
            + lax.dot_general(up[...], wu[at, :], NT, preferred_element_type=F32)
        ).astype(BF16)

    pack(3)
    own_d = ship(3)

    stores = [
        pltpu.make_async_copy(src, dst, store_sem.at[i])
        for i, (src, dst) in enumerate(
            ((rin, rin_any), (og, og_any), (hid, hid_any), (gp, gp_any), (up, up_any))
        )
    ]
    for store in stores:
        store.start()

    arrived(2, own_c)
    weight_grad[...] = jnp.zeros_like(weight_grad)

    @pl.loop(0, groups)
    def _(c):
        at = pl.ds(pl.multiple_of(c * chunk, chunk), chunk)
        got = combine(2, c)
        layer[:, at] = (weight * got).astype(BF16)
        weight_grad[...] += jnp.sum(cot[:, at].astype(F32) * got, axis=1, keepdims=True)

    for store in stores:
        store.wait()
    for p in range(3):
        left(p)
    arrived(3, own_d)

    @pl.loop(0, groups)
    def _(c):
        at = pl.ds(pl.multiple_of(c * chunk, chunk), chunk)
        row_grad[:, at] = combine(3, c).astype(BF16)

    left(3)


def local(routed_rows, expert_index, route_weight, cotangent, gate_weight, up_weight, down_weight):
    n = lax.axis_size("expert")
    row_count, width = routed_rows.shape
    units = gate_weight.shape[2]
    cap = max(2, 2 * row_count // n)
    part = math.gcd(cap, SUB)
    slab_width = (cap // part) * (width // (SUB // part))
    slots = n * cap
    tile = math.gcd(256, math.gcd(units, width))
    vmem = pl.BlockSpec(memory_space=pltpu.VMEM)
    hbm = pl.BlockSpec(memory_space=pl.ANY)
    shape = jax.ShapeDtypeStruct
    layer_out, row_grad, weight_grad, rows_in, out_grad, hidden, gate_pre, up_pre = pl.pallas_call(
        functools.partial(kernel, n, cap, part, tile),
        out_shape=(
            shape((row_count, width), BF16),
            shape((row_count, width), BF16),
            shape((row_count, 1), F32),
            shape((slots, width), BF16),
            shape((slots, width), BF16),
            shape((slots, units), BF16),
            shape((slots, units), BF16),
            shape((slots, units), BF16),
        ),
        in_specs=[vmem] * 5 + [hbm] * 3,
        out_specs=(vmem,) * 3 + (hbm,) * 5,
        scratch_shapes=[
            pltpu.VMEM((width, units), BF16),
            pltpu.VMEM((width, units), BF16),
            pltpu.VMEM((units, width), BF16),
            pltpu.VMEM((4, n * SUB, slab_width), BF16),
            pltpu.VMEM((4, n * SUB, slab_width), BF16),
            pltpu.VMEM((slots, width), BF16),
            pltpu.VMEM((slots, width), BF16),
            pltpu.VMEM((slots, units), F32),
            pltpu.VMEM((slots, units), F32),
            pltpu.VMEM((slots, units), BF16),
            pltpu.VMEM((slots, units), BF16),
            pltpu.VMEM((slots, units), BF16),
            pltpu.VMEM((slots, width), BF16),
            pltpu.SemaphoreType.DMA((3,)),
            pltpu.SemaphoreType.DMA((5,)),
            pltpu.SemaphoreType.DMA((4,)),
            pltpu.SemaphoreType.DMA((4,)),
            pltpu.SemaphoreType.DMA((4,)),
        ],
        compiler_params=pltpu.CompilerParams(
            collective_id=0, has_side_effects=True, vmem_limit_bytes=60 * 1024 * 1024
        ),
        name="routed",
    )(
        expert_index.reshape(1, row_count), expert_index, route_weight[:, None], routed_rows,
        cotangent, gate_weight[0], up_weight[0], down_weight[0],
    )
    grads = [
        lax.dot_general(a, b, TN, preferred_element_type=F32).astype(BF16)
        for a, b in ((rows_in, gate_pre), (rows_in, up_pre), (hidden, out_grad))
    ]
    return (layer_out, row_grad, weight_grad[:, 0]) + tuple(g[None] for g in grads)


def solution(mesh):
    rows, vector, cube = P("expert", None), P("expert"), P("expert", None, None)
    return jax.shard_map(
        local,
        mesh=mesh,
        in_specs=(rows, rows, vector, rows, cube, cube, cube),
        out_specs=(rows, rows, vector, cube, cube, cube),
        check_vma=False,
    )
```
